32 devices in a mesh: dp: 8 (over y, x, core), vocab: 4 (over z).
Axes of the slice: x: 2, y: 2, z: 4, core: 2. Of those that a mesh axis runs over, the one named last changes fastest.
Arguments:
- hidden: float32 [16, 4608], P('dp'), may hold values from -6 to 6
- norm_gain: float32 [4608], replicated, may hold values from 0.5 to 1.5
- embed_table: bfloat16 [12288, 4608], P(('dp', 'vocab')), as said below
- tokens: int32 [16, 3], replicated, may hold values from 0 to 12287, as said below
Outputs:
- log_probs: float32 [16, 3], P('dp')
- final_hidden: float32 [16, 4608], P('dp')
The draws below stay inside these ranges and needn't reach their ends.
Inputs may be any that keep to these rules, and one draw needn't show every extreme that they name: `tokens`: token ids are vocabulary entries. `embed_table`: entries lie between -21 / sqrt(4608) and 21 / sqrt(4608).
All inputs are finite; a program needn't handle non-finite values.
Results may differ from the reference program's by a relative error of at most 0.0003.
Values may be sent and summed in bfloat16 or wider, within the bound.
A program may use at most 64 MiB of HBM per device.

```python
import math
import jax
import jax.numpy as jnp
from jax import lax

D = 4608
VOC_DEV = 384
B_DEV = 2
STEPS = 3
B = 16
VOCAB = 12288
N_DP = 8
N_VOCAB = 4


def draw_tokens(key, part):
    key_owner = jax.random.fold_in(key, 11)
    key_local = jax.random.fold_in(key, 23)
    devices_all = N_DP * N_VOCAB
    owner = jax.random.randint(key_owner, (B, STEPS), 0, devices_all, dtype=jnp.int32)
    summary = lax_iota_rows()
    group_index = summary // B_DEV
    step_index = jnp.arange(STEPS, dtype=jnp.int32)[None, :]
    far_owner = (group_index + N_DP // 2) % N_DP * N_VOCAB + (group_index + step_index) % N_VOCAB
    chosen = jnp.where(summary % B_DEV == 0, far_owner, owner)
    local_row = jax.random.randint(key_local, (B, STEPS), 0, VOC_DEV, dtype=jnp.int32)
    return (chosen * VOC_DEV + local_row).astype(jnp.int32)


def lax_iota_rows():
    return jnp.arange(B, dtype=jnp.int32)[:, None]


def draw_embed_table(key, part):
    key_level = jax.random.fold_in(key, 31)
    key_row = jax.random.fold_in(key, 37)
    key_entry = jax.random.fold_in(key, 41)
    blocks = VOCAB // VOC_DEV
    level = jnp.exp(jax.random.uniform(key_level, (blocks, 1, 1), jnp.float32, -3.0, 0.18))
    entries = jax.random.truncated_normal(key_entry, -4.0, 4.0, (blocks, VOC_DEV, D), jnp.float32)
    row_factor = jnp.exp(jax.random.uniform(key_row, (blocks, VOC_DEV, 1), jnp.float32, -0.35, 0.35))
    table = entries * level * row_factor * (3.0 / math.sqrt(D))
    return table.reshape(VOCAB, D).astype(jnp.bfloat16)


def block_scale(own_key, extent, cuts, least, top_value):
    factor_of, own = 1.0, jax.random.fold_in(own_key, 6)
    for dim, blocks in cuts:
        steps = jnp.exp(jax.random.uniform(jax.random.fold_in(own, dim), (blocks,), jnp.float32, least / len(cuts), top_value / len(cuts)))
        factor_of = factor_of * jnp.repeat(steps, extent[dim] // blocks).reshape([-1 if axis == dim else 1 for axis in range(len(extent))])
    return factor_of


def centred(rng, shape, spread, limit, cuts=(), held_as=jnp.bfloat16):
    loudness = block_scale(rng, shape, cuts, -0.22, 0.18) if cuts else 1.0
    values = jax.random.normal(rng, shape, jnp.float32) * spread * loudness
    return jnp.minimum(jnp.maximum(values, -limit), limit).astype(held_as)


def setup_inputs(seed: int = 0) -> dict:
    keys = jax.random.split(jax.random.key(seed), 5)
    return {
        "hidden": centred(keys[0], (B, D), 1.0, 6.0, ((0, 8),), jnp.float32),
        "norm_gain": jnp.clip(1.0 + 0.1 * jax.random.normal(keys[1], (D,), jnp.float32), 0.5, 1.5),
        "embed_table": draw_embed_table(jax.random.fold_in(keys[4], 71), 0),
        "tokens": draw_tokens(jax.random.fold_in(keys[4], 71), 0),
    }


epsilon_value = 1e-06
softcap_value = 30.0

def reference(hidden, norm_gain, embed_table, tokens):
    current = hidden
    scale_factor = math.sqrt(D)
    results = []
    for decode_step in range(STEPS):
        token_ids = tokens[:, decode_step].astype(jnp.int32)
        square_mean = lax.optimization_barrier(jnp.mean(current * current, axis=-1, keepdims=True))
        normed = (current * lax.rsqrt(square_mean + epsilon_value) * norm_gain).astype(jnp.bfloat16)
        logits = lax.dot_general(normed, embed_table, (((1,), (1,)), ((), ())), preferred_element_type=jnp.float32)
        capped = softcap_value * jnp.tanh(logits / softcap_value)
        exp_total = lax.optimization_barrier(jnp.sum(jnp.exp(capped), axis=-1))
        target = jnp.take_along_axis(capped, token_ids[:, None], axis=1)[:, 0]
        results.append(target - jnp.log(exp_total))
        looked = jnp.take(embed_table, token_ids, axis=0).astype(jnp.float32)
        current = current + scale_factor * looked
    return (jnp.stack(results, axis=1), current)
```

```python
import functools
import math

import jax
import jax.numpy as jnp
from jax import lax
from jax.experimental import pallas as pl
from jax.experimental.pallas import tpu as pltpu
from jax.sharding import PartitionSpec as P

epsilon_value = 1e-06
softcap_value = 30.0
STEPS = 3
CHUNKS = 4


def each(low, high, body):
    if high - low <= 8:
        for k in range(low, high):
            body(k)
    else:
        pl.loop(low, high)(body)


def folded(low, high, body, init):
    if high - low <= 8:
        for k in range(low, high):
            init = body(k, init)
        return init
    return lax.fori_loop(low, high, body, init)


def contract(a, b):
    return lax.dot_general(a, b, (((1,), (1,)), ((), ())), preferred_element_type=jnp.float32)


def kernel(
    n_dp, n_vocab,
    hidden, gain, tokens, table, logp, final,
    tab, rows, found, found2, got_a, got_a2, part, part2, got_b, got_b2,
    state0, state1, wide0, wide1, sums, got_d,
    tab_sem, s0, r0, sa, ra, sa2, ra2, sb, rb, sb2, rb2, sc, rc, sd, rd,
):
    dp, voc = lax.axis_index("dp"), lax.axis_index("vocab")
    own, width = hidden.shape
    shard = table.shape[0]
    batch = tokens.shape[0]
    scale = math.sqrt(width)
    cut = width // CHUNKS

    loads = [
        pltpu.make_async_copy(
            table.at[:, pl.ds(i * cut, cut)], tab.at[:, pl.ds(i * cut, cut)], tab_sem.at[i]
        )
        for i in range(CHUNKS)
    ]
    for load in loads:
        load.start()

    barrier = pltpu.get_barrier_semaphore()

    def greet(k):
        pl.semaphore_signal(
            barrier, inc=1,
            device_id={"dp": lax.rem(dp + k // n_vocab, n_dp), "vocab": lax.rem(voc + k % n_vocab, n_vocab)},
            device_id_type=pl.DeviceIdType.MESH,
        )

    pl.loop(1, n_dp * n_vocab)(greet)

    def remote(src, dst, send, recv, target):
        return pltpu.make_async_remote_copy(
            src_ref=src, dst_ref=dst, send_sem=send, recv_sem=recv,
            device_id=target, device_id_type=pl.DeviceIdType.MESH,
        )

    def to_dp(k):
        return lax.rem(dp + k, n_dp)

    def from_dp(k):
        return lax.rem(dp + n_dp - k, n_dp)

    def normed_of(current):
        square_mean = jnp.mean(current * current, axis=-1, keepdims=True)
        return (current * lax.rsqrt(square_mean + epsilon_value) * gain[...]).astype(jnp.bfloat16)

    state0[dp] = normed_of(hidden[...])
    start_row = (dp * n_vocab + voc) * shard
    columns = lax.broadcasted_iota(jnp.int32, (batch, shard), 1)
    ids = tokens[...] - start_row
    matches = [columns == ids[:, s : s + 1] for s in range(STEPS)]
    onehot = jnp.concatenate(
        [jnp.where(m, 1.0, 0.0).astype(jnp.bfloat16) for m in matches], axis=0
    )

    pl.semaphore_wait(barrier, n_dp * n_vocab - 1)

    def copy0(k, slot):
        return remote(state0.at[dp], state0.at[slot], s0.at[k], r0.at[k], {"dp": to_dp(k)})

    each(1, n_dp, lambda k: copy0(k, dp).start())

    for i in range(CHUNKS):
        loads[i].wait()
        at = slice(i * cut, (i + 1) * cut)
        rows[:, at] = jnp.dot(onehot, tab[:, at], preferred_element_type=jnp.float32)
    for d in range(n_dp):
        for s in range(STEPS):
            piece = rows[s * batch + d * own : s * batch + (d + 1) * own, :].astype(jnp.bfloat16)
            if s < STEPS - 1:
                found[d, s * own : (s + 1) * own, :] = piece
            else:
                found2[d] = piece

    def copy_a(k):
        return remote(found.at[to_dp(k)], got_a.at[k], sa.at[k], ra.at[k], {"dp": to_dp(k)})

    def copy_a2(k):
        return remote(found2.at[to_dp(k)], got_a2.at[k], sa2.at[k], ra2.at[k], {"dp": to_dp(k)})

    each(1, n_dp, lambda k: copy_a(k).start())
    each(1, n_dp, lambda k: copy_a2(k).start())

    lane = lax.broadcasted_iota(jnp.int32, (batch, sums.shape[2]), 1)

    def reduced(logits, s):
        capped = softcap_value * jnp.tanh(logits / softcap_value)
        exp_total = jnp.sum(jnp.exp(capped), axis=-1, keepdims=True)
        target = jnp.sum(jnp.where(matches[s], capped, 0.0), axis=-1, keepdims=True)
        return jnp.where(lane == s, exp_total, 0.0) + jnp.where(lane == STEPS + s, target, 0.0)

    each(1, n_dp, lambda k: copy0(k, from_dp(k)).wait_recv())
    for d in range(n_dp):
        wide0[d * own : (d + 1) * own, :] = state0[d].astype(jnp.float32)
    partial = reduced(contract(wide0[...].astype(jnp.bfloat16), tab[...]), 0)

    def add_a(k, acc):
        copy_a(k).wait_recv()
        return acc + got_a[k]

    part[...] = folded(1, n_dp, add_a, found[dp])

    def copy_b(k):
        return remote(part, got_b.at[k], sb.at[k], rb.at[k], {"vocab": lax.rem(voc + k, n_vocab)})

    def copy_b2(k):
        return remote(part2, got_b2.at[k], sb2.at[k], rb2.at[k], {"vocab": lax.rem(voc + k, n_vocab)})

    each(1, n_vocab, lambda k: copy_b(k).start())

    def add_a2(k, acc):
        copy_a2(k).wait_recv()
        return acc + got_a2[k]

    part2[...] = folded(1, n_dp, add_a2, found2[dp])
    each(1, n_vocab, lambda k: copy_b2(k).start())

    def add_b(k, acc):
        copy_b(k).wait_recv()
        return acc + got_b[k]

    looked = folded(1, n_vocab, add_b, part[...]).astype(jnp.float32)
    current = hidden[...]
    for s in range(STEPS - 1):
        current = current + scale * looked[s * own : (s + 1) * own, :]
        state1[dp, s * own : (s + 1) * own, :] = normed_of(current)

    def copy_c(k, slot):
        return remote(state1.at[dp], state1.at[slot], sc.at[k], rc.at[k], {"dp": to_dp(k)})

    each(1, n_dp, lambda k: copy_c(k, dp).start())

    def add_b2(k, acc):
        copy_b2(k).wait_recv()
        return acc + got_b2[k]

    final[...] = current + scale * folded(1, n_vocab, add_b2, part2[...]).astype(jnp.float32)

    each(1, n_dp, lambda k: copy_c(k, from_dp(k)).wait_recv())
    for d in range(n_dp):
        for s in range(STEPS - 1):
            wide1[s * batch + d * own : s * batch + (d + 1) * own, :] = state1[
                d, s * own : (s + 1) * own, :
            ].astype(jnp.float32)
    logits = contract(wide1[...].astype(jnp.bfloat16), tab[...])
    for s in range(1, STEPS):
        partial = partial + reduced(logits[(s - 1) * batch : s * batch], s)
    for d in range(n_dp):
        sums[d] = partial[d * own : (d + 1) * own, :]

    def copy_d(k):
        d = lax.rem(dp + k // n_vocab, n_dp)
        v = lax.rem(voc + k % n_vocab, n_vocab)
        return remote(sums.at[d], got_d.at[k], sd.at[k], rd.at[k], {"dp": d, "vocab": v})

    pl.loop(1, n_dp * n_vocab)(lambda k: copy_d(k).start())
    got_d[0] = sums[dp]

    each(1, n_dp, lambda k: copy0(k, dp).wait_send())
    each(1, n_dp, lambda k: copy_a(k).wait_send())
    each(1, n_dp, lambda k: copy_a2(k).wait_send())
    each(1, n_vocab, lambda k: copy_b(k).wait_send())
    each(1, n_vocab, lambda k: copy_b2(k).wait_send())
    each(1, n_dp, lambda k: copy_c(k, dp).wait_send())
    pl.loop(1, n_dp * n_vocab)(lambda k: copy_d(k).wait_recv())
    total = jnp.sum(got_d[...], axis=0)
    logp[...] = total[:, STEPS : 2 * STEPS] - jnp.log(total[:, :STEPS])
    pl.loop(1, n_dp * n_vocab)(lambda k: copy_d(k).wait_send())


def on_device(n_dp, n_vocab, hidden, norm_gain, embed_table, tokens):
    own, width = hidden.shape
    shard = embed_table.shape[0]
    batch = tokens.shape[0]
    early = (STEPS - 1) * own
    bf16, f32 = jnp.bfloat16, jnp.float32
    vmem = pl.BlockSpec(memory_space=pltpu.VMEM)
    dma = pltpu.SemaphoreType.DMA
    everyone = n_dp * n_vocab
    return pl.pallas_call(
        functools.partial(kernel, n_dp, n_vocab),
        out_shape=(
            jax.ShapeDtypeStruct((own, STEPS), f32),
            jax.ShapeDtypeStruct((own, width), f32),
        ),
        in_specs=[vmem, vmem, vmem, pl.BlockSpec(memory_space=pl.ANY)],
        out_specs=(vmem, vmem),
        scratch_shapes=[
            pltpu.VMEM((shard, width), bf16),
            pltpu.VMEM((STEPS * batch, width), f32),
            pltpu.VMEM((n_dp, early, width), bf16),
            pltpu.VMEM((n_dp, own, width), bf16),
            pltpu.VMEM((n_dp, early, width), bf16),
            pltpu.VMEM((n_dp, own, width), bf16),
            pltpu.VMEM((early, width), bf16),
            pltpu.VMEM((own, width), bf16),
            pltpu.VMEM((n_vocab, early, width), bf16),
            pltpu.VMEM((n_vocab, own, width), bf16),
            pltpu.VMEM((n_dp, own, width), bf16),
            pltpu.VMEM((n_dp, early, width), bf16),
            pltpu.VMEM((batch, width), f32),
            pltpu.VMEM((early * n_dp, width), f32),
            pltpu.VMEM((n_dp, own, 128), f32),
            pltpu.VMEM((everyone, own, 128), f32),
            dma((CHUNKS,)),
            dma((n_dp,)), dma((n_dp,)),
            dma((n_dp,)), dma((n_dp,)),
            dma((n_dp,)), dma((n_dp,)),
            dma((n_vocab,)), dma((n_vocab,)),
            dma((n_vocab,)), dma((n_vocab,)),
            dma((n_dp,)), dma((n_dp,)),
            dma((everyone,)), dma((everyone,)),
        ],
        compiler_params=pltpu.CompilerParams(
            collective_id=0, has_side_effects=True, vmem_limit_bytes=48 * 1024 * 1024
        ),
    )(hidden, norm_gain.reshape(1, width), tokens, embed_table)


def solution(mesh):
    return jax.shard_map(
        functools.partial(on_device, mesh.shape["dp"], mesh.shape["vocab"]),
        mesh=mesh,
        in_specs=(P("dp", None), P(), P(("dp", "vocab"), None), P()),
        out_specs=(P("dp", None), P("dp", None)),
        check_vma=False,
    )
```

```python
import functools
import math

import jax
import jax.numpy as jnp
from jax import lax
from jax.experimental import pallas as pl
from jax.experimental.pallas import tpu as pltpu
from jax.sharding import PartitionSpec as P

epsilon_value = 1e-06
softcap_value = 30.0
STEPS = 3
CHUNKS = 4


def each(low, high, body):
    if high - low <= 8:
        for k in range(low, high):
            body(k)
    else:
        pl.loop(low, high)(body)


def folded(low, high, body, init):
    if high - low <= 8:
        for k in range(low, high):
            init = body(k, init)
        return init
    return lax.fori_loop(low, high, body, init)


def contract(a, b):
    return lax.dot_general(a, b, (((1,), (1,)), ((), ())), preferred_element_type=jnp.float32)


def kernel(
    n_dp, n_vocab,
    hidden_in, gain_in, tokens, table, logp, final,
    hidden, gain, tab, found, found2, got_a, got_a2, part, part2, got_b, got_b2,
    hidden_all, looked, base, wide, sums, got_d,
    in_sem, tab_sem, sh, rh, sa, ra, sa2, ra2, sb, rb, sb2, rb2, sc, rc, sd, rd,
):
    dp, voc = lax.axis_index("dp"), lax.axis_index("vocab")
    own, width = hidden.shape
    shard = table.shape[0]
    batch = tokens.shape[1]
    scale = math.sqrt(width)
    cut = width // CHUNKS
    early = (STEPS - 1) * own

    barrier = pltpu.get_barrier_semaphore()

    def greet(k):
        pl.semaphore_signal(
            barrier, inc=1,
            device_id={"dp": lax.rem(dp + k // n_vocab, n_dp), "vocab": lax.rem(voc + k % n_vocab, n_vocab)},
            device_id_type=pl.DeviceIdType.MESH,
        )

    pl.loop(1, n_dp * n_vocab)(greet)

    loads = [
        pltpu.make_async_copy(
            table.at[:, pl.ds(i * cut, cut)], tab.at[:, pl.ds(i * cut, cut)], tab_sem.at[i]
        )
        for i in range(CHUNKS)
    ]
    fetches = [
        pltpu.make_async_copy(hidden_in, hidden, in_sem.at[0]),
        pltpu.make_async_copy(gain_in, gain.at[0], in_sem.at[1]),
    ]
    for copy in loads + fetches:
        copy.start()

    def remote(src, dst, send, recv, target):
        return pltpu.make_async_remote_copy(
            src_ref=src, dst_ref=dst, send_sem=send, recv_sem=recv,
            device_id=target, device_id_type=pl.DeviceIdType.MESH,
        )

    def to_dp(k):
        return lax.rem(dp + k, n_dp)

    def from_dp(k):
        return lax.rem(dp + n_dp - k, n_dp)

    start_row = (dp * n_vocab + voc) * shard
    columns = lax.broadcasted_iota(jnp.int32, (batch, shard), 1)
    diagonal = lax.broadcasted_iota(jnp.int32, (batch, batch), 0) == lax.broadcasted_iota(
        jnp.int32, (batch, batch), 1
    )
    local = (tokens[...] - start_row).astype(jnp.float32)
    matches = []
    for s in range(STEPS):
        ids = jnp.sum(jnp.where(diagonal, local[s : s + 1, :], 0.0), axis=1, keepdims=True)
        matches.append(columns == ids.astype(jnp.int32))
    onehot = jnp.concatenate(
        [jnp.where(m, 1.0, 0.0).astype(jnp.bfloat16) for m in matches], axis=0
    )

    for i in range(CHUNKS):
        loads[i].wait()
        at = slice(i * cut, (i + 1) * cut)
        rows = jnp.dot(onehot, tab[:, at], preferred_element_type=jnp.float32)
        for d in range(n_dp):
            for s in range(STEPS):
                piece = rows[s * batch + d * own : s * batch + (d + 1) * own, :].astype(jnp.bfloat16)
                if s < STEPS - 1:
                    found[i, d, s * own : (s + 1) * own, :] = piece
                else:
                    found2[d, :, at] = piece
    for copy in fetches:
        copy.wait()

    pl.semaphore_wait(barrier, n_dp * n_vocab - 1)

    def copy_a(i, k):
        return remote(
            found.at[i, to_dp(k)], got_a.at[i, k], sa.at[i, k], ra.at[i, k], {"dp": to_dp(k)}
        )

    def copy_h(k, slot):
        return remote(hidden, hidden_all.at[slot], sh.at[k], rh.at[k], {"dp": to_dp(k)})

    def copy_a2(k):
        return remote(found2.at[to_dp(k)], got_a2.at[k], sa2.at[k], ra2.at[k], {"dp": to_dp(k)})

    for i in range(CHUNKS):
        each(1, n_dp, lambda k: copy_a(i, k).start())
    each(1, n_dp, lambda k: copy_h(k, dp).start())
    each(1, n_dp, lambda k: copy_a2(k).start())
    hidden_all[dp] = hidden[...]

    lane = lax.broadcasted_iota(jnp.int32, (batch, sums.shape[2]), 1)

    def reduced(logits, s):
        capped = softcap_value * jnp.tanh(logits / softcap_value)
        exp_total = jnp.sum(jnp.exp(capped), axis=-1, keepdims=True)
        target = jnp.sum(jnp.where(matches[s], capped, 0.0), axis=-1, keepdims=True)
        return jnp.where(lane == s, exp_total, 0.0) + jnp.where(lane == STEPS + s, target, 0.0)

    def normed(current, squares):
        return (current * lax.rsqrt(squares / width + epsilon_value) * gain[...]).astype(jnp.bfloat16)

    def copy_b(i, k):
        return remote(
            part.at[i], got_b.at[i, k], sb.at[i, k], rb.at[i, k], {"vocab": lax.rem(voc + k, n_vocab)}
        )

    for i in range(CHUNKS):

        def add_a(k, acc):
            copy_a(i, k).wait_recv()
            return acc + got_a[i, k]

        part[i] = folded(1, n_dp, add_a, found[i, dp])
        each(1, n_vocab, lambda k: copy_b(i, k).start())

    def copy_c(i, k, slot):
        return remote(looked.at[i, dp], looked.at[i, slot], sc.at[i, k], rc.at[i, k], {"dp": to_dp(k)})

    for i in range(CHUNKS):

        def add_b(k, acc):
            copy_b(i, k).wait_recv()
            return acc + got_b[i, k]

        looked[i, dp] = folded(1, n_vocab, add_b, part[i])
        each(1, n_dp, lambda k: copy_c(i, k, dp).start())

    def copy_b2(k):
        return remote(part2, got_b2.at[k], sb2.at[k], rb2.at[k], {"vocab": lax.rem(voc + k, n_vocab)})

    def add_a2(k, acc):
        copy_a2(k).wait_recv()
        return acc + got_a2[k]

    part2[...] = folded(1, n_dp, add_a2, found2[dp])
    each(1, n_vocab, lambda k: copy_b2(k).start())

    each(1, n_dp, lambda k: copy_h(k, from_dp(k)).wait_recv())
    for d in range(n_dp):
        base[d * own : (d + 1) * own, :] = hidden_all[d]
    first = base[...]
    partial = reduced(
        contract(normed(first, jnp.sum(first * first, axis=-1, keepdims=True)), tab[...]), 0
    )

    squares = [jnp.zeros((batch, 1), jnp.float32) for s in range(STEPS - 1)]
    for i in range(CHUNKS):
        at = slice(i * cut, (i + 1) * cut)
        each(1, n_dp, lambda k: copy_c(i, k, from_dp(k)).wait_recv())
        for d in range(n_dp):
            for s in range(STEPS - 1):
                wide[s * batch + d * own : s * batch + (d + 1) * own, at] = looked[
                    i, d, s * own : (s + 1) * own, :
                ].astype(jnp.float32)
        current = base[:, at]
        for s in range(STEPS - 1):
            current = current + scale * wide[s * batch : (s + 1) * batch, at]
            squares[s] += jnp.sum(current * current, axis=-1, keepdims=True)
            wide[s * batch : (s + 1) * batch, at] = current
    logits = contract(normed(wide[...], jnp.concatenate(squares, axis=0)), tab[...])
    for s in range(1, STEPS):
        partial = partial + reduced(logits[(s - 1) * batch : s * batch], s)
    for d in range(n_dp):
        sums[d] = partial[d * own : (d + 1) * own, :]

    def copy_d(k):
        d = lax.rem(dp + k // n_vocab, n_dp)
        v = lax.rem(voc + k % n_vocab, n_vocab)
        return remote(sums.at[d], got_d.at[k], sd.at[k], rd.at[k], {"dp": d, "vocab": v})

    pl.loop(1, n_dp * n_vocab)(lambda k: copy_d(k).start())
    got_d[0] = sums[dp]

    def add_b2(k, acc):
        copy_b2(k).wait_recv()
        return acc + got_b2[k]

    last = folded(1, n_vocab, add_b2, part2[...])
    for i in range(CHUNKS):
        at = slice(i * cut, (i + 1) * cut)
        current = hidden[:, at]
        mine = looked[i, dp].astype(jnp.float32)
        for s in range(STEPS - 1):
            current = current + scale * mine[s * own : (s + 1) * own, :]
        final[:, at] = current + scale * last[:, at].astype(jnp.float32)

    for i in range(CHUNKS):
        each(1, n_dp, lambda k: copy_a(i, k).wait_send())
        each(1, n_vocab, lambda k: copy_b(i, k).wait_send())
        each(1, n_dp, lambda k: copy_c(i, k, dp).wait_send())
    each(1, n_dp, lambda k: copy_h(k, dp).wait_send())
    each(1, n_dp, lambda k: copy_a2(k).wait_send())
    each(1, n_vocab, lambda k: copy_b2(k).wait_send())
    pl.loop(1, n_dp * n_vocab)(lambda k: copy_d(k).wait_recv())
    total = jnp.sum(got_d[...], axis=0)
    logp[...] = total[:, STEPS : 2 * STEPS] - jnp.log(total[:, :STEPS])
    pl.loop(1, n_dp * n_vocab)(lambda k: copy_d(k).wait_send())


def on_device(n_dp, n_vocab, hidden, norm_gain, embed_table, tokens):
    own, width = hidden.shape
    shard = embed_table.shape[0]
    batch = tokens.shape[0]
    early = (STEPS - 1) * own
    cut = width // CHUNKS
    bf16, f32 = jnp.bfloat16, jnp.float32
    vmem = pl.BlockSpec(memory_space=pltpu.VMEM)
    outside = pl.BlockSpec(memory_space=pl.ANY)
    dma = pltpu.SemaphoreType.DMA
    everyone = n_dp * n_vocab
    return pl.pallas_call(
        functools.partial(kernel, n_dp, n_vocab),
        out_shape=(
            jax.ShapeDtypeStruct((own, STEPS), f32),
            jax.ShapeDtypeStruct((own, width), f32),
        ),
        in_specs=[outside, outside, vmem, outside],
        out_specs=(vmem, vmem),
        scratch_shapes=[
            pltpu.VMEM((own, width), f32),
            pltpu.VMEM((1, width), f32),
            pltpu.VMEM((shard, width), bf16),
            pltpu.VMEM((CHUNKS, n_dp, early, cut), bf16),
            pltpu.VMEM((n_dp, own, width), bf16),
            pltpu.VMEM((CHUNKS, n_dp, early, cut), bf16),
            pltpu.VMEM((n_dp, own, width), bf16),
            pltpu.VMEM((CHUNKS, early, cut), bf16),
            pltpu.VMEM((own, width), bf16),
            pltpu.VMEM((CHUNKS, n_vocab, early, cut), bf16),
            pltpu.VMEM((n_vocab, own, width), bf16),
            pltpu.VMEM((n_dp, own, width), f32),
            pltpu.VMEM((CHUNKS, n_dp, early, cut), bf16),
            pltpu.VMEM((batch, width), f32),
            pltpu.VMEM((early * n_dp, width), f32),
            pltpu.VMEM((n_dp, own, 128), f32),
            pltpu.VMEM((everyone, own, 128), f32),
            dma((2,)), dma((CHUNKS,)),
            dma((n_dp,)), dma((n_dp,)),
            dma((CHUNKS, n_dp)), dma((CHUNKS, n_dp)),
            dma((n_dp,)), dma((n_dp,)),
            dma((CHUNKS, n_vocab)), dma((CHUNKS, n_vocab)),
            dma((n_vocab,)), dma((n_vocab,)),
            dma((CHUNKS, n_dp)), dma((CHUNKS, n_dp)),
            dma((everyone,)), dma((everyone,)),
        ],
        compiler_params=pltpu.CompilerParams(
            collective_id=0, has_side_effects=True, vmem_limit_bytes=60 * 1024 * 1024
        ),
    )(hidden, norm_gain, jnp.transpose(tokens), embed_table)


def solution(mesh):
    return jax.shard_map(
        functools.partial(on_device, mesh.shape["dp"], mesh.shape["vocab"]),
        mesh=mesh,
        in_specs=(P("dp", None), P(), P(("dp", "vocab"), None), P()),
        out_specs=(P("dp", None), P("dp", None)),
        check_vma=False,
    )
```
